32 devices in a mesh: dp: 16 (over z, y, core), expert: 2 (over x).
Axes of the slice: x: 2, y: 2, z: 4, core: 2. Of those that a mesh axis runs over, the one named last changes fastest.
Arguments:
- tokens: bfloat16 [256, 6144], P('dp', 'expert'), may hold values from -6 to 6
- expert_ids: int32 [256, 2], P('dp'), may hold values from 0 to 7, all different within a row; in each aligned block of 16 rows (0 to 15, 16 to 31, ...) at most 8 rows name the same one
- gate_probs: float32 [256, 2], P('dp'), may hold values from 0.1 to 1
- w_gate: bfloat16 [8, 6144, 8192], P('expert', None, 'dp'), may hold values from -0.078125 to 0.078125
- w_up: bfloat16 [8, 6144, 8192], P('expert', None, 'dp'), may hold values from -0.078125 to 0.078125
- w_down_t: bfloat16 [8, 6144, 8192], P('expert', 'dp'), may hold values from -0.0625 to 0.0625
Outputs:
- mixed: bfloat16 [256, 6144], P('dp', 'expert')
The draws below stay inside these ranges and needn't reach their ends.
Inputs may be any that keep to these rules, and one draw needn't show every extreme that they name: `expert_ids`: each row names 2 different experts. Among the 16 rows of one index of dp no expert is named more than 8 times, a bound that some block reaches.
All inputs are finite; a program needn't handle non-finite values.
Results may differ from the reference program's by a relative error of at most 0.0057.
Values may be sent and summed in bfloat16 or wider, within the bound.
A program may use at most 128 MiB of HBM per device.

```python
import math
import jax
import jax.numpy as jnp
import numpy as np
from jax import lax

D = 6144
FF = 8192
EXPERTS = 8
TOP = 2
TOK_DEV = 16
CAP = 8
TOKENS = 256
N_DP = 16


def shard_levels(stream_key, dims, pieces, smallest, high):
    factor_of = 1.0
    for dim, shards_of in pieces:
        steps = jax.random.uniform(jax.random.fold_in(jax.random.fold_in(stream_key, 6), dim), (shards_of,), jnp.float32, smallest / len(pieces), high / len(pieces))
        factor_of = factor_of * jnp.repeat(jnp.exp(steps), dims[dim] // shards_of).reshape((-1,) + (1,) * (len(dims) - 1 - dim))
    return factor_of


def deal_out(key, own, number, rows, count, top, most, lean):
    order = jax.random.permutation(key, count)
    packed, ordinary = load_shares(count, rows * top, most, lean, True), load_shares(count, rows * top, most, lean, False)
    places = jnp.arange(count)

    def named(tallies, turn):
        used = int((tallies > 0).sum())
        fixed = max(1, used // 4)
        passed = fixed + (places - fixed + turn * (used - fixed)) % max(1, count - fixed)
        return jnp.zeros((count,), jnp.int32).at[order[jnp.where(places < fixed, places, passed)]].set(jnp.asarray(tallies, jnp.int32))

    tallies = jnp.where(number % 4 == 0, named(packed, number // 4), named(ordinary, number - number // 4 - 1))
    mixed = jax.random.permutation(jax.random.fold_in(own, 3), count)
    source_of, taker = mixed[0:count // 2 * 2:2], mixed[1:count // 2 * 2:2]
    slack = jnp.minimum(tallies[source_of] - 1, most - tallies[taker]) // 2
    slack = jnp.where((source_of == order[0]) | (taker == order[0]) | (tallies[taker] == 0), 0, jnp.maximum(slack, 0))
    passed = jax.random.randint(jax.random.fold_in(own, 4), (count // 2,), 0, 1 << 20) % (slack + 1)
    tallies = tallies.at[source_of].add(-passed).at[taker].add(passed)
    labels = jnp.searchsorted(jnp.cumsum(tallies), jnp.arange(rows * top), side="right").astype(jnp.int32)
    table = labels.reshape(top, rows).T
    table = table[jax.random.permutation(jax.random.fold_in(own, 1), rows)]
    turn = jax.random.randint(jax.random.fold_in(own, 2), (rows, 1), 0, top)
    return jnp.take_along_axis(table, (jnp.arange(top)[None, :] + turn) % top, axis=1)


def load_shares(number_of, total, limit, skew, full):
    portions = [(1 << 20) // math.isqrt(standing ** skew) + 1 for standing in range(1, number_of + 1)]
    largest = limit if full else min(limit, max(-(-total // number_of), total * portions[0] // sum(portions)))
    least = 1 if total - largest >= number_of - 1 else 0
    counts, rest = [largest] + [least] * (number_of - 1), total - largest - least * (number_of - 1)
    while rest > 0:
        free = [i for i in range(1, number_of) if counts[i] < largest] or [i for i in range(1, number_of) if counts[i] < limit]
        pool, remaining = sum([portions[i] for i in free]), rest
        for i in free:
            more = min(limit - counts[i], max(1, remaining * portions[i] // pool), rest)
            counts[i] = counts[i] + more
            rest = rest - more
    return np.array(counts)


def normal_values(own_key, shape, spread, limit, split=(), kind=jnp.bfloat16):
    array = spread * jax.random.normal(own_key, shape, jnp.float32)
    if split:
        array = array * shard_levels(own_key, shape, split, -0.22, 0.18)
    return jnp.clip(array, -limit, limit).astype(kind)


def setup_inputs(seed: int = 0) -> dict:
    key_list = jax.random.split(jax.random.key(seed), 7)
    tokens = normal_values(key_list[0], (TOKENS, D), 1.0, 6.0, ((0, 16), (1, 2)))
    expert_ids_keys = jax.random.split(jax.random.fold_in(key_list[1], 1), TOKENS // TOK_DEV)
    expert_ids_turns = jax.random.permutation(jax.random.fold_in(key_list[1], 3), TOKENS // TOK_DEV)
    expert_ids = jax.vmap(lambda own, number: deal_out(jax.random.fold_in(key_list[1], 2), own, number, TOK_DEV, EXPERTS, TOP, CAP, 2))(expert_ids_keys, expert_ids_turns).reshape((TOKENS, TOP))
    gate_probs = jnp.clip(jnp.exp(math.log(1.0) - 2.3025851 * jax.random.uniform(key_list[2], (TOKENS, TOP), jnp.float32) ** shard_levels(key_list[2], (TOKENS, TOP), ((0, 16),), -0.2, 0.2)), 0.1, 1.0)
    w_gate = normal_values(key_list[3], (EXPERTS, D, FF), D ** -0.5, 0.078125, ((0, 2), (2, 16)))
    w_up = normal_values(key_list[4], (EXPERTS, D, FF), D ** -0.5, 0.078125, ((0, 2), (2, 16)))
    w_down_t = normal_values(key_list[5], (EXPERTS, D, FF), FF ** -0.5, 0.0625, ((0, 2), (1, 16)))
    return dict(tokens=tokens, expert_ids=expert_ids, gate_probs=gate_probs, w_gate=w_gate, w_up=w_up, w_down_t=w_down_t)


def positions(expert_ids):
    blocks = expert_ids.reshape(N_DP, TOK_DEV * TOP)
    onehot = (blocks[:, :, None] == jnp.arange(EXPERTS, dtype=jnp.int32)[None, None, :]).astype(jnp.int32)
    earlier = jnp.cumsum(onehot, axis=1) - onehot
    return jnp.sum(earlier * onehot, axis=2).reshape(TOKENS, TOP).astype(jnp.int32)


def one_expert(operands):
    rows, gate_w, up_w, down_w = operands
    gate = jnp.dot(rows, gate_w, preferred_element_type=jnp.float32)
    up = jnp.dot(rows, up_w, preferred_element_type=jnp.float32)
    hidden = (jax.nn.silu(gate) * up).astype(jnp.bfloat16)
    result = lax.dot_general(hidden, down_w, (((1,), (1,)), ((), ())), preferred_element_type=jnp.float32)
    return result.astype(jnp.bfloat16)


def reference(tokens, expert_ids, gate_probs, w_gate, w_up, w_down_t):
    position = positions(expert_ids)
    block_of = (jnp.arange(TOKENS, dtype=jnp.int32) // TOK_DEV).astype(jnp.int32)
    block_rep = jnp.repeat(block_of, TOP)
    flat_ids = expert_ids.reshape(-1).astype(jnp.int32)
    flat_pos = position.reshape(-1).astype(jnp.int32)
    dispatched = jnp.zeros((EXPERTS, N_DP, CAP, D), jnp.bfloat16)
    dispatched = dispatched.at[flat_ids, block_rep, flat_pos].set(jnp.repeat(tokens, TOP, axis=0))
    expert_out = lax.map(one_expert, (dispatched.reshape(EXPERTS, N_DP * CAP, D), w_gate, w_up, w_down_t))
    expert_out = expert_out.reshape(EXPERTS, N_DP, CAP, D)
    picked = expert_out[flat_ids, block_rep, flat_pos].reshape(TOKENS, TOP, D).astype(jnp.float32)
    mixed = jnp.sum(gate_probs[:, :, None] * picked, axis=1)
    return mixed.astype(jnp.bfloat16)
```

```python
import functools

import jax
import jax.numpy as jnp
from jax import lax
from jax.experimental import pallas as pl
from jax.experimental.pallas import tpu as pltpu
from jax.sharding import PartitionSpec as P


def assignments(expert_ids, experts, capacity):
    flat = expert_ids.reshape(-1)
    onehot = (flat[:, None] == jnp.arange(experts, dtype=jnp.int32)[None, :]).astype(jnp.int32)
    earlier = jnp.cumsum(onehot, axis=0) - onehot
    position = jnp.sum(earlier * onehot, axis=1).reshape(expert_ids.shape)
    expert_hit = (
        expert_ids[:, :, None] == jnp.arange(experts, dtype=jnp.int32)[None, None, :]
    ).astype(jnp.float32)
    slot_hit = (
        position[:, :, None] == jnp.arange(capacity, dtype=jnp.int32)[None, None, :]
    ).astype(jnp.float32)
    return (expert_hit, slot_hit)


def gathered(tokens, expert_ids, gate_probs, w_gate, w_up, w_down_t):
    local_experts = w_gate.shape[0]
    expert_count = lax.axis_size("expert")
    dp_count = lax.axis_size("dp")
    experts = local_experts * expert_count
    capacity = tokens.shape[0] // 2
    expert_hit, slot_hit = assignments(expert_ids, experts, capacity)
    dispatch_map = jnp.einsum("tke,tkc->ect", expert_hit, slot_hit).astype(jnp.bfloat16)
    combine_map = jnp.einsum(
        "tk,tke,tkc->tec", gate_probs, expert_hit, slot_hit, precision=lax.Precision.HIGHEST
    )
    slots = jnp.einsum(
        "ect,td->ecd", dispatch_map, tokens, preferred_element_type=jnp.float32
    ).astype(jnp.bfloat16)
    arrived = lax.all_to_all(slots, "expert", split_axis=0, concat_axis=2, tiled=True)
    piece = lax.all_gather(arrived, "dp", axis=1, tiled=True)
    gate = jnp.einsum("erd,edf->erf", piece, w_gate, preferred_element_type=jnp.float32)
    up = jnp.einsum("erd,edf->erf", piece, w_up, preferred_element_type=jnp.float32)
    hidden = (jax.nn.silu(gate) * up).astype(jnp.bfloat16)
    partial_out = jnp.einsum(
        "erf,edf->erd",
        lax.all_gather(hidden, "dp", axis=2, tiled=True),
        w_down_t,
        preferred_element_type=jnp.float32,
    )
    results = partial_out.astype(jnp.bfloat16).reshape(
        local_experts, dp_count, capacity, w_down_t.shape[1]
    )
    results = lax.all_to_all(results, "dp", split_axis=1, concat_axis=3, tiled=True)
    results = results.reshape(local_experts, capacity, results.shape[3])
    slice_width = tokens.shape[1]
    outgoing = results.reshape(local_experts, capacity, expert_count, slice_width)
    returned = lax.all_to_all(outgoing, "expert", split_axis=2, concat_axis=0, tiled=True)
    returned = returned.reshape(experts, capacity, slice_width)
    mixed = jnp.einsum(
        "tec,ecd->td", combine_map, returned.astype(jnp.float32), precision=lax.Precision.HIGHEST
    )
    return mixed.astype(jnp.bfloat16)


MESH = pl.DeviceIdType.MESH
META = 128


def fused(
    shape,
    packed, w_gate, w_up, w_down, out,
    tok, hid, xbuf, wg, wu, wd, acc, total, pbuf, fin,
    x_send, x_recv, own_sem,
    t_ring_send, t_ring_recv, t_part_send, t_part_recv,
    h_ring_send, h_ring_recv, h_part_send, h_part_recv,
    w_sem, d_sem, f_send, f_recv,
):
    experts, chips, block, capacity, half = shape
    dp, x = lax.axis_index("dp"), lax.axis_index("expert")
    chip, core = dp // 2, dp % 2
    odd = chip % 2
    place = (1 - odd) * (chip // 2) + odd * (chips - 1 - chip // 2)

    def chip_at(position):
        p = (position + chips) % chips
        back = p // (chips // 2)
        return (1 - back) * (2 * p) + back * (2 * (chips - 1 - p) + 1)

    right = (chip_at(place + 1) * 2 + core, x)
    left = (chip_at(place - 1) * 2 + core, x)
    partner = (chip * 2 + 1 - core, x)
    opposite = (dp, 1 - x)

    def send(src, dst, send_sem, recv_sem, device):
        pltpu.make_async_remote_copy(
            src_ref=src, dst_ref=dst, send_sem=send_sem, recv_sem=recv_sem,
            device_id=device, device_id_type=MESH,
        ).start()

    def wait(ref, sem):
        pltpu.make_async_copy(ref, ref, sem).wait()

    def hops(q, way):
        longer = chips // 2
        return longer if q % 2 == way else chips - 1 - longer

    def ring(buffer, index, ring_send, ring_recv, part_send, part_recv):
        def own(q, src):
            dst = buffer.at[index(q), core, chip]
            send(src, dst, ring_send.at[q], ring_recv.at[q, 0, 0], right)
            send(src, dst, ring_send.at[q], ring_recv.at[q, 1, 0], left)
            send(src, dst, part_send.at[q], part_recv.at[q], partner)

        def serve(q, hop):
            for way in range(2):
                count = hops(q, way)
                if hop > count:
                    continue
                origin = chip_at(place - hop if way == 0 else place + hop)
                arrived = buffer.at[index(q), core, origin]
                wait(arrived, ring_recv.at[q, way, hop - 1])
                if hop < count:
                    send(
                        arrived, arrived, ring_send.at[q], ring_recv.at[q, way, hop],
                        right if way == 0 else left,
                    )
                send(arrived, arrived, part_send.at[q], part_recv.at[q], partner)

        def others(q):
            wait(buffer.at[index(q), 1 - core], part_recv.at[q])

        def sent(q):
            wait(buffer.at[index(q), core, pl.ds(0, chips - 1)], ring_send.at[q])
            wait(buffer.at[index(q), core], part_send.at[q])

        return own, serve, others, sent

    def load_up(e):
        s = e % 2
        pltpu.make_async_copy(w_gate.at[e], wg.at[s], w_sem.at[0, s]).start()
        pltpu.make_async_copy(w_up.at[e], wu.at[s], w_sem.at[1, s]).start()

    def load_down(e):
        pltpu.make_async_copy(w_down.at[e], wd.at[e % 2], d_sem.at[e % 2]).start()

    longest = chips // 2

    own, serve, others, sent = ring(
        tok, lambda q: x if q == 0 else 1 - x,
        t_ring_send, t_ring_recv, t_part_send, t_part_recv,
    )
    send(packed, tok.at[x, core, chip], x_send, x_recv, opposite)
    own(0, packed)
    pltpu.make_async_copy(packed, tok.at[x, core, chip], own_sem).start()
    for e in range(min(2, experts)):
        load_up(e)
    wait(tok.at[1 - x, core, chip], x_recv)
    own(1, tok.at[1 - x, core, chip])
    for hop in range(1, longest + 1):
        serve(0, hop)
        serve(1, hop)
    wait(packed, x_send)
    pltpu.make_async_copy(packed, tok.at[x, core, chip], own_sem).wait()
    for q in range(2):
        others(q)
        sent(q)

    blocks = 2 * chips
    tokens, rows = blocks * block, blocks * capacity
    meta = tok[0, :, :, :, half:half + META].reshape(tokens, META).astype(jnp.float32)
    token_of = lax.broadcasted_iota(jnp.int32, (tokens, rows), 0)
    slot_of = lax.broadcasted_iota(jnp.int32, (tokens, rows), 1)
    same_block = (token_of // block) == (slot_of // capacity)
    slot_in = slot_of % capacity

    def weights(e):
        key = ((x * experts + e) * capacity + slot_in).astype(jnp.float32)
        hit = [jnp.where(same_block & (meta[:, k:k + 1] == key), 1.0, 0.0) for k in range(2)]
        prob = [meta[:, 2 + k:3 + k] + meta[:, 4 + k:5 + k] + meta[:, 6 + k:7 + k] for k in range(2)]
        return hit[0] + hit[1], hit[0] * prob[0] + hit[1] * prob[1]

    tile = half // 3 if half % 384 == 0 else half
    per_half = half // tile
    units = wg.shape[2]
    width = 256 if units % 256 == 0 else units

    def compute_up(e):
        s = e % 2
        chosen = weights(e)[0].astype(jnp.bfloat16)

        @pl.loop(0, 2 * per_half)
        def _(k):
            first = pl.multiple_of((k % per_half) * tile, 128)
            piece = tok[k // per_half, :, :, :, pl.ds(first, tile)].reshape(tokens, tile)
            picked = lax.dot_general(
                chosen, piece, (((0,), (0,)), ((), ())), preferred_element_type=jnp.float32
            )
            xbuf[:, pl.ds(pl.multiple_of(k * tile, 128), tile)] = picked.astype(jnp.bfloat16)

        wait(wg.at[s], w_sem.at[0, s])
        wait(wu.at[s], w_sem.at[1, s])

        @pl.loop(0, units // width)
        def _(n):
            columns = pl.ds(pl.multiple_of(n * width, 128), width)
            gate = jnp.dot(xbuf[...], wg[s, :, columns], preferred_element_type=jnp.float32)
            up = jnp.dot(xbuf[...], wu[s, :, columns], preferred_element_type=jnp.float32)
            hidden = gate / (1.0 + jnp.exp(-gate)) * up
            hid[e, core, chip, :, columns] = hidden.astype(jnp.bfloat16)

    def compute_down(e):
        s = e % 2
        wait(wd.at[s], d_sem.at[s])
        acc[...] = jnp.zeros_like(acc)

        @pl.loop(0, blocks)
        def _(b):
            first = ((b % chips) * 2 + b // chips) * units
            acc[...] += lax.dot_general(
                hid[e, b // chips, b % chips],
                wd[s, :, pl.ds(pl.multiple_of(first, 128), units)],
                (((1,), (1,)), ((), ())), preferred_element_type=jnp.float32,
            )

        result = acc[...].astype(jnp.bfloat16)
        weight = weights(e)[1]
        high = weight.astype(jnp.bfloat16)
        low = (weight - high.astype(jnp.float32)).astype(jnp.bfloat16)
        term = jnp.dot(high, result, preferred_element_type=jnp.float32)
        term = term + jnp.dot(low, result, preferred_element_type=jnp.float32)
        if e == 0:
            total[...] = term
        else:
            total[...] += term

    own, serve, others, sent = ring(
        hid, lambda e: e, h_ring_send, h_ring_recv, h_part_send, h_part_recv
    )
    for stage in range(experts + longest):
        if stage < experts:
            compute_up(stage)
            own(stage, hid.at[stage, core, chip])
            if stage + 2 < experts:
                load_up(stage + 2)
            if stage == experts - 1:
                for e in range(min(2, experts)):
                    load_down(e)
        for e in range(experts):
            if 1 <= stage - e <= longest:
                serve(e, stage - e)
        e = stage - longest
        if e >= 0:
            others(e)
            compute_down(e)
            if e + 2 < experts:
                load_down(e + 2)

    pbuf[...] = total[...].astype(jnp.bfloat16).reshape(pbuf.shape)
    side, lane = dp // chips, dp % chips
    slot = lane * 2 + x
    here = side == x
    for step in range(1, blocks):
        j = (dp + step) % blocks
        send(pbuf.at[j % 2, j // 2], fin.at[slot], f_send.at[step], f_recv.at[slot], (j, side))

    mine = pbuf.at[core, chip]

    @pl.when(here)
    def _():
        pltpu.make_async_copy(mine, fin.at[slot], f_send.at[0]).start()
        pltpu.make_async_copy(mine, fin.at[slot], f_send.at[0]).wait()

    @pl.when(jnp.logical_not(here))
    def _():
        send(mine, fin.at[slot], f_send.at[0], f_recv.at[slot], (dp, side))
        wait(mine, f_send.at[0])

    for e in range(experts):
        sent(e)
    for source in range(blocks):
        from_here = here & (slot == source)

        @pl.when(jnp.logical_not(from_here))
        def _():
            wait(fin.at[source], f_recv.at[source])

    features = fin.shape[2]
    for i in range(chips):
        both = fin[2 * i].astype(jnp.float32) + fin[2 * i + 1].astype(jnp.float32)
        out[:, i * features:(i + 1) * features] = both.astype(jnp.bfloat16)
    for step in range(1, blocks):
        j = (dp + step) % blocks
        wait(pbuf.at[j % 2, j // 2], f_send.at[step])


def per_device(tokens, expert_ids, gate_probs, w_gate, w_up, w_down_t):
    experts, depth, units = w_gate.shape
    block, half = tokens.shape
    features, wide = w_down_t.shape[1:]
    dp_count, expert_count = lax.axis_size("dp"), lax.axis_size("expert")
    capacity = block // 2
    chips = dp_count // 2
    fits = (
        expert_count == 2 and chips >= 4 and chips % 2 == 0 and block == 16
        and half % 128 == 0 and units % 128 == 0 and features % 128 == 0
        and chips * capacity * 2 % 128 == 0 and 8 * experts * depth * units <= 2 ** 27
    )
    if not fits:
        return gathered(tokens, expert_ids, gate_probs, w_gate, w_up, w_down_t)
    flat = expert_ids.reshape(-1)
    same = (flat[:, None] == flat[None, :]) & (
        jnp.arange(2 * block)[:, None] > jnp.arange(2 * block)[None, :]
    )
    position = jnp.sum(same.astype(jnp.int32), axis=1).reshape(expert_ids.shape)
    slots = (expert_ids * capacity + position).astype(jnp.float32)
    high = lax.reduce_precision(gate_probs, 8, 7)
    middle = lax.reduce_precision(gate_probs - high, 8, 7)
    low = gate_probs - high - middle
    meta = jnp.concatenate([slots, high, middle, low], axis=1).astype(jnp.bfloat16)
    meta = jnp.pad(meta, ((0, 0), (0, META - meta.shape[1])))
    packed = jnp.concatenate([tokens, meta], axis=1)

    longest = chips // 2
    rows = dp_count * capacity
    bf, dma = jnp.bfloat16, pltpu.SemaphoreType.DMA
    vmem, anywhere = pl.BlockSpec(memory_space=pltpu.VMEM), pl.BlockSpec(memory_space=pl.ANY)
    return pl.pallas_call(
        functools.partial(fused, (experts, chips, block, capacity, half)),
        out_shape=jax.ShapeDtypeStruct((block, half), bf),
        in_specs=[vmem, anywhere, anywhere, anywhere],
        out_specs=vmem,
        scratch_shapes=[
            pltpu.VMEM((2, 2, chips, block, half + META), bf),
            pltpu.VMEM((experts, 2, chips, rows, units), bf),
            pltpu.VMEM((rows, depth), bf),
            pltpu.VMEM((2, depth, units), bf),
            pltpu.VMEM((2, depth, units), bf),
            pltpu.VMEM((2, features, wide), bf),
            pltpu.VMEM((rows, features), jnp.float32),
            pltpu.VMEM((dp_count * block, features), jnp.float32),
            pltpu.VMEM((2, chips, block, features), bf),
            pltpu.VMEM((dp_count, block, features), bf),
            dma, dma, dma,
            dma((2,)), dma((2, 2, longest)), dma((2,)), dma((2,)),
            dma((experts,)), dma((experts, 2, longest)), dma((experts,)), dma((experts,)),
            dma((2, 2)), dma((2,)), dma((dp_count,)), dma((dp_count,)),
        ],
        compiler_params=pltpu.CompilerParams(
            has_side_effects=True, vmem_limit_bytes=62 * 2 ** 20
        ),
        name="fused_experts",
    )(packed, w_gate, w_up, w_down_t)


def solution(mesh):
    placed = (
        P("dp", "expert"),
        P("dp", None),
        P("dp", None),
        P("expert", None, "dp"),
        P("expert", None, "dp"),
        P("expert", "dp", None),
    )
    return jax.shard_map(
        per_device, mesh=mesh, in_specs=placed, out_specs=P("dp", "expert"), check_vma=False
    )
```

```python
import functools

import jax
import jax.numpy as jnp
from jax import lax
from jax.experimental import pallas as pl
from jax.experimental.pallas import tpu as pltpu
from jax.sharding import PartitionSpec as P


def assignments(expert_ids, experts, capacity):
    flat = expert_ids.reshape(-1)
    onehot = (flat[:, None] == jnp.arange(experts, dtype=jnp.int32)[None, :]).astype(jnp.int32)
    earlier = jnp.cumsum(onehot, axis=0) - onehot
    position = jnp.sum(earlier * onehot, axis=1).reshape(expert_ids.shape)
    expert_hit = (
        expert_ids[:, :, None] == jnp.arange(experts, dtype=jnp.int32)[None, None, :]
    ).astype(jnp.float32)
    slot_hit = (
        position[:, :, None] == jnp.arange(capacity, dtype=jnp.int32)[None, None, :]
    ).astype(jnp.float32)
    return (expert_hit, slot_hit)


def gathered(tokens, expert_ids, gate_probs, w_gate, w_up, w_down_t):
    local_experts = w_gate.shape[0]
    expert_count = lax.axis_size("expert")
    dp_count = lax.axis_size("dp")
    experts = local_experts * expert_count
    capacity = tokens.shape[0] // 2
    expert_hit, slot_hit = assignments(expert_ids, experts, capacity)
    dispatch_map = jnp.einsum("tke,tkc->ect", expert_hit, slot_hit).astype(jnp.bfloat16)
    combine_map = jnp.einsum(
        "tk,tke,tkc->tec", gate_probs, expert_hit, slot_hit, precision=lax.Precision.HIGHEST
    )
    slots = jnp.einsum(
        "ect,td->ecd", dispatch_map, tokens, preferred_element_type=jnp.float32
    ).astype(jnp.bfloat16)
    arrived = lax.all_to_all(slots, "expert", split_axis=0, concat_axis=2, tiled=True)
    piece = lax.all_gather(arrived, "dp", axis=1, tiled=True)
    gate = jnp.einsum("erd,edf->erf", piece, w_gate, preferred_element_type=jnp.float32)
    up = jnp.einsum("erd,edf->erf", piece, w_up, preferred_element_type=jnp.float32)
    hidden = (jax.nn.silu(gate) * up).astype(jnp.bfloat16)
    partial_out = jnp.einsum(
        "erf,edf->erd",
        lax.all_gather(hidden, "dp", axis=2, tiled=True),
        w_down_t,
        preferred_element_type=jnp.float32,
    )
    results = partial_out.astype(jnp.bfloat16).reshape(
        local_experts, dp_count, capacity, w_down_t.shape[1]
    )
    results = lax.all_to_all(results, "dp", split_axis=1, concat_axis=3, tiled=True)
    results = results.reshape(local_experts, capacity, results.shape[3])
    slice_width = tokens.shape[1]
    outgoing = results.reshape(local_experts, capacity, expert_count, slice_width)
    returned = lax.all_to_all(outgoing, "expert", split_axis=2, concat_axis=0, tiled=True)
    returned = returned.reshape(experts, capacity, slice_width)
    mixed = jnp.einsum(
        "tec,ecd->td", combine_map, returned.astype(jnp.float32), precision=lax.Precision.HIGHEST
    )
    return mixed.astype(jnp.bfloat16)


MESH = pl.DeviceIdType.MESH
META = 128


def fused(
    shape,
    packed, w_gate, w_up, w_down, out,
    tok, hid, xbuf, wg, wu, wd, acc, total, pbuf, fin,
    x_send, x_recv, own_sem,
    t_ring_send, t_ring_recv, t_part_send, t_part_recv,
    h_ring_send, h_ring_recv, h_part_send, h_part_recv,
    w_sem, d_sem, f_send, f_recv,
):
    experts, chips, block, capacity, half = shape
    dp, x = lax.axis_index("dp"), lax.axis_index("expert")
    chip, core = dp // 2, dp % 2
    odd = chip % 2
    place = (1 - odd) * (chip // 2) + odd * (chips - 1 - chip // 2)

    def chip_at(position):
        p = (position + chips) % chips
        back = p // (chips // 2)
        return (1 - back) * (2 * p) + back * (2 * (chips - 1 - p) + 1)

    right = (chip_at(place + 1) * 2 + core, x)
    left = (chip_at(place - 1) * 2 + core, x)
    partner = (chip * 2 + 1 - core, x)
    opposite = (dp, 1 - x)

    def send(src, dst, send_sem, recv_sem, device):
        pltpu.make_async_remote_copy(
            src_ref=src, dst_ref=dst, send_sem=send_sem, recv_sem=recv_sem,
            device_id=device, device_id_type=MESH,
        ).start()

    def wait(ref, sem):
        pltpu.make_async_copy(ref, ref, sem).wait()

    def hops(q, way):
        longer = chips // 2
        return longer if q % 2 == way else chips - 1 - longer

    def ring(buffer, index, ring_send, ring_recv, part_send, part_recv):
        def own(q, src):
            dst = buffer.at[index(q), core, chip]
            send(src, dst, ring_send.at[q], ring_recv.at[q, 0, 0], right)
            send(src, dst, ring_send.at[q], ring_recv.at[q, 1, 0], left)
            send(src, dst, part_send.at[q], part_recv.at[q], partner)

        def serve(q, hop):
            for way in range(2):
                count = hops(q, way)
                if hop > count:
                    continue
                origin = chip_at(place - hop if way == 0 else place + hop)
                arrived = buffer.at[index(q), core, origin]
                wait(arrived, ring_recv.at[q, way, hop - 1])
                if hop < count:
                    send(
                        arrived, arrived, ring_send.at[q], ring_recv.at[q, way, hop],
                        right if way == 0 else left,
                    )
                send(arrived, arrived, part_send.at[q], part_recv.at[q], partner)

        def others(q):
            wait(buffer.at[index(q), 1 - core], part_recv.at[q])

        def sent(q):
            wait(buffer.at[index(q), core, pl.ds(0, chips - 1)], ring_send.at[q])
            wait(buffer.at[index(q), core], part_send.at[q])

        return own, serve, others, sent

    def load_up(e):
        s = e % 2
        pltpu.make_async_copy(w_gate.at[e], wg.at[s], w_sem.at[0, s]).start()
        pltpu.make_async_copy(w_up.at[e], wu.at[s], w_sem.at[1, s]).start()

    def load_down(e):
        pltpu.make_async_copy(w_down.at[e], wd.at[e % 2], d_sem.at[e % 2]).start()

    longest = chips // 2

    own, serve, others, sent = ring(
        tok, lambda q: x if q == 0 else 1 - x,
        t_ring_send, t_ring_recv, t_part_send, t_part_recv,
    )
    send(packed, tok.at[x, core, chip], x_send, x_recv, opposite)
    own(0, packed)
    pltpu.make_async_copy(packed, tok.at[x, core, chip], own_sem).start()
    for e in range(min(2, experts)):
        load_up(e)
    wait(tok.at[1 - x, core, chip], x_recv)
    own(1, tok.at[1 - x, core, chip])
    for hop in range(1, longest + 1):
        serve(0, hop)
        serve(1, hop)
    wait(packed, x_send)
    pltpu.make_async_copy(packed, tok.at[x, core, chip], own_sem).wait()
    for q in range(2):
        others(q)
        sent(q)

    blocks = 2 * chips
    tokens, rows = blocks * block, blocks * capacity
    meta = tok[0, :, :, :, half:half + META].reshape(tokens, META).astype(jnp.float32)
    token_of = lax.broadcasted_iota(jnp.int32, (tokens, rows), 0)
    slot_of = lax.broadcasted_iota(jnp.int32, (tokens, rows), 1)
    same_block = (token_of // block) == (slot_of // capacity)
    slot_in = slot_of % capacity

    def weights(e):
        key = ((x * experts + e) * capacity + slot_in).astype(jnp.float32)
        hit = [jnp.where(same_block & (meta[:, k:k + 1] == key), 1.0, 0.0) for k in range(2)]
        prob = [meta[:, 2 + k:3 + k] + meta[:, 4 + k:5 + k] + meta[:, 6 + k:7 + k] for k in range(2)]
        return hit[0] + hit[1], hit[0] * prob[0] + hit[1] * prob[1]

    tile = half // 3 if half % 384 == 0 else half
    per_half = half // tile
    units = wg.shape[2]
    width = 256 if units % 256 == 0 else units

    def compute_up(e):
        s = e % 2
        chosen = weights(e)[0].astype(jnp.bfloat16)

        @pl.loop(0, 2 * per_half, unroll=2)
        def _(k):
            first = pl.multiple_of((k % per_half) * tile, 128)
            piece = tok[k // per_half, :, :, :, pl.ds(first, tile)].reshape(tokens, tile)
            picked = lax.dot_general(
                chosen, piece, (((0,), (0,)), ((), ())), preferred_element_type=jnp.float32
            )
            xbuf[:, pl.ds(pl.multiple_of(k * tile, 128), tile)] = picked.astype(jnp.bfloat16)

        wait(wg.at[s], w_sem.at[0, s])
        wait(wu.at[s], w_sem.at[1, s])

        @pl.loop(0, units // width)
        def _(n):
            columns = pl.ds(pl.multiple_of(n * width, 128), width)
            gate = jnp.dot(xbuf[...], wg[s, :, columns], preferred_element_type=jnp.float32)
            up = jnp.dot(xbuf[...], wu[s, :, columns], preferred_element_type=jnp.float32)
            hidden = gate / (1.0 + jnp.exp(-gate)) * up
            hid[e, core, chip, :, columns] = hidden.astype(jnp.bfloat16)

    def compute_down(e):
        s = e % 2
        wait(wd.at[s], d_sem.at[s])
        acc[...] = jnp.zeros_like(acc)

        @pl.loop(0, blocks, unroll=4)
        def _(b):
            first = ((b % chips) * 2 + b // chips) * units
            acc[...] += lax.dot_general(
                hid[e, b // chips, b % chips],
                wd[s, :, pl.ds(pl.multiple_of(first, 128), units)],
                (((1,), (1,)), ((), ())), preferred_element_type=jnp.float32,
            )

        result = acc[...].astype(jnp.bfloat16)
        weight = weights(e)[1]
        high = weight.astype(jnp.bfloat16)
        low = (weight - high.astype(jnp.float32)).astype(jnp.bfloat16)
        term = jnp.dot(high, result, preferred_element_type=jnp.float32)
        term = term + jnp.dot(low, result, preferred_element_type=jnp.float32)
        if e == 0:
            total[...] = term
        else:
            total[...] += term

    own, serve, others, sent = ring(
        hid, lambda e: e, h_ring_send, h_ring_recv, h_part_send, h_part_recv
    )
    for stage in range(experts + longest):
        if stage < experts:
            compute_up(stage)
            own(stage, hid.at[stage, core, chip])
            if stage + 2 < experts:
                load_up(stage + 2)
            if stage == experts - 1:
                for e in range(min(2, experts)):
                    load_down(e)
        for e in range(experts):
            if 1 <= stage - e <= longest:
                serve(e, stage - e)
        e = stage - longest
        if e >= 0:
            others(e)
            compute_down(e)
            if e + 2 < experts:
                load_down(e + 2)

    pbuf[...] = total[...].astype(jnp.bfloat16).reshape(pbuf.shape)
    side, lane = dp // chips, dp % chips
    slot = lane * 2 + x
    here = side == x
    for step in range(1, blocks):
        j = (dp + step) % blocks
        send(pbuf.at[j % 2, j // 2], fin.at[slot], f_send.at[step], f_recv.at[slot], (j, side))

    mine = pbuf.at[core, chip]

    @pl.when(here)
    def _():
        pltpu.make_async_copy(mine, fin.at[slot], f_send.at[0]).start()
        pltpu.make_async_copy(mine, fin.at[slot], f_send.at[0]).wait()

    @pl.when(jnp.logical_not(here))
    def _():
        send(mine, fin.at[slot], f_send.at[0], f_recv.at[slot], (dp, side))
        wait(mine, f_send.at[0])

    for e in range(experts):
        sent(e)
    for source in range(blocks):
        from_here = here & (slot == source)

        @pl.when(jnp.logical_not(from_here))
        def _():
            wait(fin.at[source], f_recv.at[source])

    features = fin.shape[2]
    for i in range(chips):
        both = fin[2 * i].astype(jnp.float32) + fin[2 * i + 1].astype(jnp.float32)
        out[:, i * features:(i + 1) * features] = both.astype(jnp.bfloat16)
    for step in range(1, blocks):
        j = (dp + step) % blocks
        wait(pbuf.at[j % 2, j // 2], f_send.at[step])


def per_device(tokens, expert_ids, gate_probs, w_gate, w_up, w_down_t):
    experts, depth, units = w_gate.shape
    block, half = tokens.shape
    features, wide = w_down_t.shape[1:]
    dp_count, expert_count = lax.axis_size("dp"), lax.axis_size("expert")
    capacity = block // 2
    chips = dp_count // 2
    fits = (
        expert_count == 2 and chips >= 4 and chips % 2 == 0 and block == 16
        and half % 128 == 0 and units % 128 == 0 and features % 128 == 0
        and chips * capacity * 2 % 128 == 0 and 8 * experts * depth * units <= 2 ** 27
    )
    if not fits:
        return gathered(tokens, expert_ids, gate_probs, w_gate, w_up, w_down_t)
    flat = expert_ids.reshape(-1)
    same = (flat[:, None] == flat[None, :]) & (
        jnp.arange(2 * block)[:, None] > jnp.arange(2 * block)[None, :]
    )
    position = jnp.sum(same.astype(jnp.int32), axis=1).reshape(expert_ids.shape)
    slots = (expert_ids * capacity + position).astype(jnp.float32)
    high = lax.reduce_precision(gate_probs, 8, 7)
    middle = lax.reduce_precision(gate_probs - high, 8, 7)
    low = gate_probs - high - middle
    meta = jnp.concatenate([slots, high, middle, low], axis=1).astype(jnp.bfloat16)
    meta = jnp.pad(meta, ((0, 0), (0, META - meta.shape[1])))
    packed = jnp.concatenate([tokens, meta], axis=1)

    longest = chips // 2
    rows = dp_count * capacity
    bf, dma = jnp.bfloat16, pltpu.SemaphoreType.DMA
    vmem, anywhere = pl.BlockSpec(memory_space=pltpu.VMEM), pl.BlockSpec(memory_space=pl.ANY)
    return pl.pallas_call(
        functools.partial(fused, (experts, chips, block, capacity, half)),
        out_shape=jax.ShapeDtypeStruct((block, half), bf),
        in_specs=[vmem, anywhere, anywhere, anywhere],
        out_specs=vmem,
        scratch_shapes=[
            pltpu.VMEM((2, 2, chips, block, half + META), bf),
            pltpu.VMEM((experts, 2, chips, rows, units), bf),
            pltpu.VMEM((rows, depth), bf),
            pltpu.VMEM((2, depth, units), bf),
            pltpu.VMEM((2, depth, units), bf),
            pltpu.VMEM((2, features, wide), bf),
            pltpu.VMEM((rows, features), jnp.float32),
            pltpu.VMEM((dp_count * block, features), jnp.float32),
            pltpu.VMEM((2, chips, block, features), bf),
            pltpu.VMEM((dp_count, block, features), bf),
            dma, dma, dma,
            dma((2,)), dma((2, 2, longest)), dma((2,)), dma((2,)),
            dma((experts,)), dma((experts, 2, longest)), dma((experts,)), dma((experts,)),
            dma((2, 2)), dma((2,)), dma((dp_count,)), dma((dp_count,)),
        ],
        compiler_params=pltpu.CompilerParams(
            has_side_effects=True, vmem_limit_bytes=62 * 2 ** 20
        ),
        name="fused_experts",
    )(packed, w_gate, w_up, w_down_t)


def solution(mesh):
    placed = (
        P("dp", "expert"),
        P("dp", None),
        P("dp", None),
        P("expert", None, "dp"),
        P("expert", None, "dp"),
        P("expert", "dp", None),
    )
    return jax.shard_map(
        per_device, mesh=mesh, in_specs=placed, out_specs=P("dp", "expert"), check_vma=False
    )
```
